16 devices in a mesh: dp: 2 (over z), tp: 8 (over y, x, core).
Axes of the slice: x: 2, y: 2, z: 2, core: 2. Of those that a mesh axis runs over, the one named last changes fastest.
Arguments:
- x: bfloat16 [16, 768, 4096], P('dp'), parts along dimension 0
- seq_lens: int32 [16], P('dp'), parts along dimension 0
- w_query: bfloat16 [4096, 4096], P(None, 'tp')
- w_key: bfloat16 [4096, 1024], P(None, 'tp')
- w_value: bfloat16 [4096, 1024], P(None, 'tp')
- w_out: bfloat16 [4096, 4096], P('tp')
- w_gate: bfloat16 [4096, 14336], P(None, 'tp')
- w_up: bfloat16 [4096, 14336], P(None, 'tp')
- w_down: bfloat16 [14336, 4096], P('tp')
- attn_gain: bfloat16 [4096], replicated
- mlp_gain: bfloat16 [4096], replicated
- k_cache: bfloat16 [16, 1536, 8, 128], P('dp', None, 'tp'), parts along dimension 0
- v_cache: bfloat16 [16, 1536, 8, 128], P('dp', None, 'tp'), parts along dimension 0
Outputs:
- output 1: bfloat16 [16, 768, 4096], P('dp'), parts along dimension 0
- output 2: bfloat16 [16, 1536, 8, 128], P('dp', None, 'tp'), parts along dimension 0
- output 3: bfloat16 [16, 1536, 8, 128], P('dp', None, 'tp'), parts along dimension 0
There are 2 independent parts. The reference program is written for one: setup_inputs(seed, part) draws one part's arguments, and reference() takes and returns one part's arrays. A program takes and returns all parts, laid end to end along the dimension named above; an argument that names none is the same for every part.
All inputs are finite; a program needn't handle non-finite values.
Results may differ from the reference program's by a relative error of at most 0.0114972.
Values are sent between devices in bfloat16 or wider.
A program may use at most 1 GiB of HBM per device.

```python
import jax
import jax.numpy as jnp
from jax import lax

D = 4096
HEADS = 32
KV_HEADS = 8
HEAD = 128
FF = 14336
BATCH = 8
SEQ = 768
CACHE_LEN = 1536
TP = 8
EPS = 1e-5
ROPE_BASE = 10000.0


def setup_inputs(seed: int = 0, part: int = 0) -> dict:
    base_key = jax.random.key(seed)
    part_key = jax.random.fold_in(base_key, part)
    weight_keys = jax.random.split(base_key, 9)
    part_keys = jax.random.split(part_key, 5)
    qk_scale = 1.5 * D ** -0.5

    def normal_weight(rng_key, array_shape, factor):
        return (jax.random.normal(rng_key, array_shape, jnp.float32) * factor).astype(jnp.bfloat16)

    short_len = jax.random.randint(part_keys[1], (1,), SEQ // 2, (4 * SEQ) // 5 + 1)
    other_lens = jax.random.randint(part_keys[2], (BATCH - 1,), SEQ // 2, SEQ + 1)
    return {
        "x": normal_weight(part_keys[0], (BATCH, SEQ, D), 1.0),
        "seq_lens": jnp.concatenate([short_len, other_lens]).astype(jnp.int32),
        "w_query": normal_weight(weight_keys[0], (D, HEADS * HEAD), qk_scale),
        "w_key": normal_weight(weight_keys[1], (D, KV_HEADS * HEAD), qk_scale),
        "w_value": normal_weight(weight_keys[2], (D, KV_HEADS * HEAD), D ** -0.5),
        "w_out": normal_weight(weight_keys[3], (HEADS * HEAD, D), (HEADS * HEAD) ** -0.5),
        "w_gate": normal_weight(weight_keys[4], (D, FF), D ** -0.5),
        "w_up": normal_weight(weight_keys[5], (D, FF), D ** -0.5),
        "w_down": normal_weight(weight_keys[6], (FF, D), FF ** -0.5),
        "attn_gain": jax.random.uniform(weight_keys[7], (D,), jnp.float32, 0.5, 1.5).astype(jnp.bfloat16),
        "mlp_gain": jax.random.uniform(weight_keys[8], (D,), jnp.float32, 0.5, 1.5).astype(jnp.bfloat16),
        "k_cache": normal_weight(part_keys[3], (BATCH, CACHE_LEN, KV_HEADS, HEAD), 1.0),
        "v_cache": normal_weight(part_keys[4], (BATCH, CACHE_LEN, KV_HEADS, HEAD), 1.0),
    }


def rms_norm(rows, gain):
    rows32 = rows.astype(jnp.float32)
    inv_rms = lax.rsqrt(jnp.mean(rows32 * rows32, axis=-1, keepdims=True) + EPS)
    return (rows32 * inv_rms * gain.astype(jnp.float32)).astype(jnp.bfloat16)


def rotary(vecs, angles):
    half_dim = HEAD // 2
    pairs = vecs.reshape(vecs.shape[:-1] + (half_dim, 2))
    even_part = pairs[..., 0]
    odd_part = pairs[..., 1]
    cos_tab = jnp.cos(angles)[:, None, :]
    sin_tab = jnp.sin(angles)[:, None, :]
    turned = jnp.stack([even_part * cos_tab - odd_part * sin_tab, even_part * sin_tab + odd_part * cos_tab], axis=-1)
    return turned.reshape(vecs.shape)


def reference(x, seq_lens, w_query, w_key, w_value, w_out, w_gate, w_up, w_down, attn_gain, mlp_gain, k_cache, v_cache):
    group_size = HEADS // KV_HEADS
    heads_part = HEADS * HEAD // TP
    ff_part = FF // TP
    positions = jnp.arange(SEQ)
    inv_freq = ROPE_BASE ** (-jnp.arange(0, HEAD, 2).astype(jnp.float32) / HEAD)
    angles = positions.astype(jnp.float32)[:, None] * inv_freq[None, :]
    causal = positions[None, :] <= positions[:, None]

    def one_sequence(items):
        x_row, length = items
        normed = rms_norm(x_row, attn_gain)
        queries = rotary(jnp.dot(normed, w_query, preferred_element_type=jnp.float32).reshape(SEQ, HEADS, HEAD), angles).astype(jnp.bfloat16)
        keys = rotary(jnp.dot(normed, w_key, preferred_element_type=jnp.float32).reshape(SEQ, KV_HEADS, HEAD), angles).astype(jnp.bfloat16)
        values = jnp.dot(normed, w_value, preferred_element_type=jnp.float32).astype(jnp.bfloat16).reshape(SEQ, KV_HEADS, HEAD)
        valid = positions < length
        keys = jnp.where(valid[:, None, None], keys, jnp.zeros_like(keys))
        values = jnp.where(valid[:, None, None], values, jnp.zeros_like(values))
        allowed = causal & valid[None, :]

        def one_kv_head(blocks):
            q_block, k_block, v_block = blocks
            scores = jnp.einsum("qgh,sh->gqs", q_block.astype(jnp.float32), k_block.astype(jnp.float32)) * HEAD ** -0.5
            scores = jnp.where(allowed[None], scores, -jnp.inf)
            probs = jax.nn.softmax(scores, axis=-1).astype(jnp.bfloat16)
            mixed = jnp.einsum("gqs,sh->qgh", probs.astype(jnp.float32), v_block.astype(jnp.float32))
            return mixed.astype(jnp.bfloat16)

        q_grouped = jnp.transpose(queries.reshape(SEQ, KV_HEADS, group_size, HEAD), (1, 0, 2, 3))
        head_out = lax.map(one_kv_head, (q_grouped, jnp.transpose(keys, (1, 0, 2)), jnp.transpose(values, (1, 0, 2))))
        attn_rows = jnp.transpose(head_out, (1, 0, 2, 3)).reshape(SEQ, HEADS * HEAD)
        attn_sum = jnp.zeros((SEQ, D), jnp.float32)
        for index in range(TP):
            partial = jnp.dot(attn_rows[:, index * heads_part:(index + 1) * heads_part], w_out[index * heads_part:(index + 1) * heads_part], preferred_element_type=jnp.float32)
            attn_sum = attn_sum + partial.astype(jnp.bfloat16).astype(jnp.float32)
        hidden = (x_row.astype(jnp.float32) + attn_sum).astype(jnp.bfloat16)
        normed_mlp = rms_norm(hidden, mlp_gain)
        gate_pre = jnp.dot(normed_mlp, w_gate, preferred_element_type=jnp.float32)
        up_pre = jnp.dot(normed_mlp, w_up, preferred_element_type=jnp.float32)
        gated = (jax.nn.silu(gate_pre) * up_pre).astype(jnp.bfloat16)
        mlp_sum = jnp.zeros((SEQ, D), jnp.float32)
        for index in range(TP):
            partial = jnp.dot(gated[:, index * ff_part:(index + 1) * ff_part], w_down[index * ff_part:(index + 1) * ff_part], preferred_element_type=jnp.float32)
            mlp_sum = mlp_sum + partial.astype(jnp.bfloat16).astype(jnp.float32)
        out_row = (hidden.astype(jnp.float32) + mlp_sum).astype(jnp.bfloat16)
        return out_row, keys, values

    y, new_keys, new_values = lax.map(one_sequence, (x, seq_lens))
    k_cache_out = lax.dynamic_update_slice(k_cache, new_keys, (0, 0, 0, 0))
    v_cache_out = lax.dynamic_update_slice(v_cache, new_values, (0, 0, 0, 0))
    return y, k_cache_out, v_cache_out
```

```python
import functools

import jax
import jax.numpy as jnp
from jax import lax
from jax.experimental import pallas as pl
from jax.experimental.pallas import tpu as pltpu
from jax.sharding import PartitionSpec as P

EPS = 1e-5
ROPE_BASE = 10000.0
F32 = jnp.float32
BF16 = jnp.bfloat16
CHUNK = 2
TILE = 256


def rms_rows(rows, gain):
    rows32 = rows.astype(F32)
    inv_rms = lax.rsqrt(jnp.mean(rows32 * rows32, axis=-1, keepdims=True) + EPS)
    return (rows32 * inv_rms * gain.astype(F32)).astype(BF16)


def qkv_kernel(tiles, lens_ref, x_ref, gain_ref, wq_ref, wkv_ref, cos_ref, sin_ref, q_ref, k_ref, v_ref):
    step = pl.program_id(0)
    normed = rms_rows(x_ref[...], gain_ref[...])
    head = cos_ref.shape[1]
    cos_tab = cos_ref[...]
    sin_tab = sin_ref[...]
    even = lax.broadcasted_iota(jnp.int32, cos_tab.shape, 1) % 2 == 0

    def turn(part):
        swapped = jnp.where(even, pltpu.roll(part, head - 1, 1), pltpu.roll(part, 1, 1))
        return (part * cos_tab + swapped * sin_tab).astype(BF16)

    kv = jnp.dot(normed, wkv_ref[...], preferred_element_type=F32)
    rows = lax.rem(step, tiles) * cos_tab.shape[0] + lax.broadcasted_iota(jnp.int32, cos_tab.shape, 0)
    valid = rows < lens_ref[step // tiles]
    zero = jnp.zeros(cos_tab.shape, BF16)
    k_ref[...] = jnp.where(valid, turn(kv[:, :head]), zero)
    v_ref[...] = jnp.where(valid, kv[:, head:].astype(BF16), zero)
    queries = jnp.dot(normed, wq_ref[...], preferred_element_type=F32)
    for h in range(queries.shape[1] // head):
        cols = slice(h * head, (h + 1) * head)
        q_ref[:, cols] = turn(queries[:, cols])


def attention_kernel(first, lens_ref, q_ref, k_ref, v_ref, o_ref):
    length = lens_ref[first + pl.program_id(0)]
    seq_len, head = k_ref.shape
    scale = head ** -0.5
    for tile in range(seq_len // TILE):
        width = (tile + 1) * TILE
        rows = slice(tile * TILE, (tile + 1) * TILE)
        query_at = tile * TILE + lax.broadcasted_iota(jnp.int32, (TILE, width), 0)
        key_at = lax.broadcasted_iota(jnp.int32, (TILE, width), 1)
        allowed = (key_at <= query_at) & (key_at < length)
        for h in range(q_ref.shape[1] // head):
            cols = slice(h * head, (h + 1) * head)
            scores = lax.dot_general(q_ref[rows, cols], k_ref[:width, :], (((1,), (1,)), ((), ())), preferred_element_type=F32)
            scores = jnp.where(allowed, scores * scale, -jnp.inf)
            top = jnp.max(scores, axis=-1, keepdims=True)
            weights = jnp.exp(scores - top)
            probs = (weights / jnp.sum(weights, axis=-1, keepdims=True)).astype(BF16)
            o_ref[rows, cols] = jnp.dot(probs, v_ref[:width, :], preferred_element_type=F32).astype(BF16)


def out_kernel(core_ref, o_ref, w_ref, x_ref, gain_ref, h_ref, n_ref, total):
    step = pl.program_id(1)

    @pl.when(step == 0)
    def _():
        total[...] = jnp.zeros_like(total)

    part = jnp.dot(o_ref[0], w_ref[...], preferred_element_type=F32).astype(BF16)
    total[...] += part.astype(F32)

    @pl.when(step == pl.num_programs(1) - 1)
    def _():
        hidden = (x_ref[...].astype(F32) + total[...]).astype(BF16)
        h_ref[...] = hidden
        n_ref[...] = rms_rows(hidden, gain_ref[...])


def rope_tables(seq_len, head):
    inv_freq = ROPE_BASE ** (-jnp.arange(0, head, 2).astype(F32) / head)
    angles = jnp.arange(seq_len).astype(F32)[:, None] * inv_freq[None, :]
    sign = jnp.where(jnp.arange(head) % 2 == 0, -1.0, 1.0).astype(F32)
    return jnp.repeat(jnp.cos(angles), 2, axis=1), jnp.repeat(jnp.sin(angles), 2, axis=1) * sign


def vmem_limit(mib):
    return dict(vmem_limit_bytes=mib * 2 ** 20)


def project_qkv(x_rows, gain, w_query, w_kv, seq_lens, seq_len, head):
    rows, width = x_rows.shape
    tiles = seq_len // TILE
    cos_tab, sin_tab = rope_tables(seq_len, head)
    whole = lambda shape: pl.BlockSpec(shape, lambda i, s: (0, 0))
    table = pl.BlockSpec((TILE, head), lambda i, s: (lax.rem(i, tiles), 0))
    by_row = lambda cols: pl.BlockSpec((TILE, cols), lambda i, s: (i, 0))
    q_cols = w_query.shape[1]
    return pl.pallas_call(
        functools.partial(qkv_kernel, tiles),
        grid_spec=pltpu.PrefetchScalarGridSpec(
            num_scalar_prefetch=1, grid=(rows // TILE,),
            in_specs=[by_row(width), whole((1, width)), whole(w_query.shape), whole(w_kv.shape), table, table],
            out_specs=[by_row(q_cols), by_row(head), by_row(head)]),
        out_shape=[jax.ShapeDtypeStruct((rows, q_cols), BF16)] + [jax.ShapeDtypeStruct((rows, head), BF16)] * 2,
        compiler_params=pltpu.CompilerParams(**vmem_limit(56)),
        cost_estimate=pl.CostEstimate(flops=2 * rows * width * (q_cols + 2 * head), bytes_accessed=2 * rows * width, transcendentals=0),
    )(seq_lens, x_rows, gain.reshape(1, -1), w_query, w_kv, cos_tab, sin_tab)


def attend(queries, keys, values, seq_lens, first, count, seq_len):
    q_cols, head = queries.shape[1], keys.shape[1]
    by_seq = lambda cols: pl.BlockSpec((seq_len, cols), lambda i, s: (first + i, 0))
    return pl.pallas_call(
        functools.partial(attention_kernel, first),
        grid_spec=pltpu.PrefetchScalarGridSpec(
            num_scalar_prefetch=1, grid=(count,),
            in_specs=[by_seq(q_cols), by_seq(head), by_seq(head)],
            out_specs=pl.BlockSpec((seq_len, q_cols), lambda i, s: (i, 0))),
        out_shape=jax.ShapeDtypeStruct((count * seq_len, q_cols), BF16),
        compiler_params=pltpu.CompilerParams(**vmem_limit(48)),
        cost_estimate=pl.CostEstimate(flops=count * 8 * 10 ** 9, bytes_accessed=count * 2 * 10 ** 6, transcendentals=0),
    )(seq_lens, queries, keys, values)


def project_out(gathered, w_full, x_rows, gain, core, first, rows):
    groups, _, group_cols = gathered.shape
    width = w_full.shape[1]
    tile = rows // 2
    per = rows // tile
    row_block = pl.BlockSpec((tile, width), lambda r, i, c: (r, 0))
    return pl.pallas_call(
        out_kernel,
        grid_spec=pltpu.PrefetchScalarGridSpec(
            num_scalar_prefetch=1, grid=(per, groups),
            in_specs=[pl.BlockSpec((1, tile, group_cols), lambda r, i, c: (i, c[0] * per + r, 0)),
                      pl.BlockSpec((group_cols, width), lambda r, i, c: (i, 0)),
                      pl.BlockSpec((tile, width), lambda r, i, c: (first * per + c[0] * per + r, 0)),
                      pl.BlockSpec((1, width), lambda r, i, c: (0, 0))],
            out_specs=[row_block, row_block],
            scratch_shapes=[pltpu.VMEM((tile, width), F32)]),
        out_shape=[jax.ShapeDtypeStruct((rows, width), BF16)] * 2,
        compiler_params=pltpu.CompilerParams(**vmem_limit(56)),
        cost_estimate=pl.CostEstimate(flops=2 * rows * width * groups * group_cols, bytes_accessed=4 * width * width, transcendentals=0),
    )(core, gathered, w_full, x_rows, gain.reshape(1, -1))


def solution(mesh):
    tp_size = mesh.shape["tp"]
    sibling = [(i, i ^ 1) for i in range(tp_size)]
    first_axis = [(i, i ^ (4 if i % 2 else 2)) for i in range(tp_size)]
    second_axis = [(i, i ^ (2 if i % 2 else 4)) for i in range(tp_size)]
    swap = lambda value, pairs: lax.ppermute(value, "tp", pairs)

    def layer_shard(x, seq_lens, w_query, w_key, w_value, w_out, w_gate, w_up, w_down, attn_gain, mlp_gain, k_cache, v_cache):
        batch_size, seq_len, width = x.shape
        head = k_cache.shape[3]
        half = width // 2
        block = seq_len // 2
        me = lax.axis_index("tp")
        core = me % 2
        at_x = (me // 2) % 2
        at_y = me // 4
        bit_first = jnp.where(core == 0, at_x, at_y)
        bit_second = jnp.where(core == 0, at_y, at_x)
        pick = lambda value, index, axis=0: lax.dynamic_index_in_dim(value, index, axis, keepdims=False)

        w_full = lax.all_gather(w_out, "tp", axis=0, tiled=True)
        x_rows = x.reshape(batch_size * seq_len, width)
        queries, keys, values = project_qkv(x_rows, attn_gain, w_query, jnp.concatenate([w_key, w_value], axis=1), seq_lens, seq_len, head)
        as_cache = lambda rows: rows.reshape(batch_size, seq_len, 1, head)
        k_cache_out = lax.dynamic_update_slice(k_cache, as_cache(keys), (0, 0, 0, 0))
        v_cache_out = lax.dynamic_update_slice(v_cache, as_cache(values), (0, 0, 0, 0))
        halves = w_down.reshape(-1, 2, half)
        down_own = pick(halves, core, 1)
        down_other = pick(halves, 1 - core, 1)
        core_arg = core.astype(jnp.int32).reshape(1)

        outs = []
        for first in range(0, batch_size, CHUNK):
            attn = attend(queries, keys, values, seq_lens, first, CHUNK, seq_len)
            gathered = lax.all_gather(attn, "tp", axis=0)
            hidden, normed = project_out(gathered, w_full, x_rows, mlp_gain, core_arg, first, seq_len)
            normed_other = swap(normed, sibling)
            normed_both = jnp.stack([jnp.where(core == 0, normed, normed_other), jnp.where(core == 0, normed_other, normed)])
            hidden_parts = hidden.reshape(2, block, 2, half)
            give = pick(pick(hidden_parts, bit_first), 1 - core, 1)
            take = swap(give, sibling)
            hidden_mine = jnp.where(bit_first == core, pick(pick(hidden_parts, bit_second), core, 1), take)
            normed_rows = normed_both.reshape(2 * seq_len, width)
            gate_pre = jnp.dot(normed_rows, w_gate, preferred_element_type=F32)
            up_pre = jnp.dot(normed_rows, w_up, preferred_element_type=F32)
            gated = (jax.nn.silu(gate_pre) * up_pre).astype(BF16)
            part_other = jnp.dot(gated, down_other, preferred_element_type=F32).astype(BF16)
            from_sibling = swap(part_other, sibling)
            part_own = lax.reduce_precision(jnp.dot(gated, down_own, preferred_element_type=F32), 8, 7)
            pair = (part_own + from_sibling.astype(F32)).reshape(2, seq_len, half)
            quad = pick(pair, bit_first) + swap(pick(pair, 1 - bit_first), first_axis)
            quad = quad.reshape(2, block, half)
            total = pick(quad, bit_second) + swap(pick(quad, 1 - bit_second), second_axis)
            outs.append((hidden_mine.astype(F32) + total).astype(BF16))

        y = jnp.zeros_like(x)
        for index, rows in enumerate(outs):
            blocks = lax.all_gather(rows, "tp", axis=0).reshape(2, 2, 2, block, half)
            left = jnp.transpose(blocks[:, :, 0], (1, 0, 2, 3))
            piece = jnp.concatenate([left, blocks[:, :, 1]], axis=-1).reshape(CHUNK, seq_len, width)
            y = lax.dynamic_update_slice(y, piece, (index * CHUNK, 0, 0))
        return y, k_cache_out, v_cache_out

    cache_spec = P("dp", None, "tp", None)
    return jax.shard_map(layer_shard, mesh=mesh, in_specs=(P("dp", None, None), P("dp"), P(None, "tp"), P(None, "tp"), P(None, "tp"), P("tp", None), P(None, "tp"), P(None, "tp"), P("tp", None), P(), P(), cache_spec, cache_spec), out_specs=(P("dp", None, None), cache_spec, cache_spec), check_vma=False)
```

```python
import functools

import jax
import jax.numpy as jnp
from jax import lax
from jax.experimental import pallas as pl
from jax.experimental.pallas import tpu as pltpu
from jax.sharding import PartitionSpec as P


EPS = 1e-5
ROPE_BASE = 10000.0
F32 = jnp.float32
BF16 = jnp.bfloat16
PIECES = (1,2,2,2,1)
TILE = 256


def rms_rows(rows, gain):
    rows32 = rows.astype(F32)
    inv_rms = lax.rsqrt(jnp.mean(rows32 * rows32, axis=-1, keepdims=True) + EPS)
    return (rows32 * inv_rms * gain.astype(F32)).astype(BF16)


def qkv_kernel(tiles, lens_ref, x_ref, gain_ref, wq_ref, wkv_ref, cos_ref, sin_ref, q_ref, k_ref, v_ref):
    step = pl.program_id(0)
    normed = rms_rows(x_ref[...], gain_ref[...])
    head = cos_ref.shape[1]
    cos_tab = cos_ref[...]
    sin_tab = sin_ref[...]
    even = lax.broadcasted_iota(jnp.int32, cos_tab.shape, 1) % 2 == 0

    def turn(part):
        swapped = jnp.where(even, pltpu.roll(part, head - 1, 1), pltpu.roll(part, 1, 1))
        return (part * cos_tab + swapped * sin_tab).astype(BF16)

    kv = jnp.dot(normed, wkv_ref[...], preferred_element_type=F32)
    rows = lax.rem(step, tiles) * cos_tab.shape[0] + lax.broadcasted_iota(jnp.int32, cos_tab.shape, 0)
    valid = rows < lens_ref[step // tiles]
    zero = jnp.zeros(cos_tab.shape, BF16)
    k_ref[...] = jnp.where(valid, turn(kv[:, :head]), zero)
    v_ref[...] = jnp.where(valid, kv[:, head:].astype(BF16), zero)
    queries = jnp.dot(normed, wq_ref[...], preferred_element_type=F32)
    for h in range(queries.shape[1] // head):
        cols = slice(h * head, (h + 1) * head)
        q_ref[:, cols] = turn(queries[:, cols])


def attention_kernel(lens_ref, seq_ref, q_ref, k_ref, v_ref, *o_refs):
    step = pl.program_id(0)
    length = lens_ref[seq_ref[step]]
    seq_len, head = k_ref.shape
    scale = head ** -0.5

    def run(o_ref):
        for tile in range(seq_len // TILE):
            width = (tile + 1) * TILE
            rows = slice(tile * TILE, (tile + 1) * TILE)
            query_at = tile * TILE + lax.broadcasted_iota(jnp.int32, (TILE, width), 0)
            key_at = lax.broadcasted_iota(jnp.int32, (TILE, width), 1)
            allowed = (key_at <= query_at) & (key_at < length)
            for h in range(q_ref.shape[1] // head):
                cols = slice(h * head, (h + 1) * head)
                scores = lax.dot_general(q_ref[rows, cols], k_ref[:width, :], (((1,), (1,)), ((), ())), preferred_element_type=F32)
                scores = jnp.where(allowed, scores * scale, -jnp.inf)
                top = jnp.max(scores, axis=-1, keepdims=True)
                weights = jnp.exp(scores - top)
                probs = (weights / jnp.sum(weights, axis=-1, keepdims=True)).astype(BF16)
                o_ref[rows, cols] = jnp.dot(probs, v_ref[:width, :], preferred_element_type=F32).astype(BF16)

    for which, o_ref in enumerate(o_refs):
        @pl.when(step == which)
        def _():
            run(o_ref)


def out_kernel(place_ref, *refs):
    pairs, (w_ref, x_ref, gain_ref, h_ref, n_ref, total) = refs[:-6], refs[-6:]
    step = pl.program_id(0)
    core = place_ref[0]
    depth = w_ref.shape[0] // 2
    tile = x_ref.shape[0]
    at_rows = pl.ds(pl.multiple_of(pl.program_id(1) * tile, tile), tile)
    cols = 1024

    for which, o_ref in enumerate(pairs):
        @pl.when(step == which)
        def _():
            for col in range(0, total.shape[1], cols):
                at = slice(col, col + cols)
                own = jnp.dot(o_ref[:, :depth], w_ref[pl.ds(pl.multiple_of(core * depth, depth), depth), at], preferred_element_type=F32).astype(BF16)
                other = jnp.dot(o_ref[:, depth:], w_ref[pl.ds(pl.multiple_of((1 - core) * depth, depth), depth), at], preferred_element_type=F32).astype(BF16)
                both = own.astype(F32) + other.astype(F32)
                total[at_rows, at] = both if which == 0 else total[at_rows, at] + both

    @pl.when(step == pl.num_programs(0) - 1)
    def _():
        hidden = (x_ref[...].astype(F32) + total[at_rows, :]).astype(BF16)
        h_ref[...] = hidden
        n_ref[...] = rms_rows(hidden, gain_ref[...])


def rope_tables(seq_len, head):
    inv_freq = ROPE_BASE ** (-jnp.arange(0, head, 2).astype(F32) / head)
    angles = jnp.arange(seq_len).astype(F32)[:, None] * inv_freq[None, :]
    sign = jnp.where(jnp.arange(head) % 2 == 0, -1.0, 1.0).astype(F32)
    return jnp.repeat(jnp.cos(angles), 2, axis=1), jnp.repeat(jnp.sin(angles), 2, axis=1) * sign


def vmem_limit(mib):
    return dict(vmem_limit_bytes=mib * 2 ** 20)


def project_qkv(x_rows, gain, w_query, w_kv, seq_lens, seq_len, head):
    rows, width = x_rows.shape
    tiles = seq_len // TILE
    cos_tab, sin_tab = rope_tables(seq_len, head)
    whole = lambda shape: pl.BlockSpec(shape, lambda i, s: (0, 0))
    table = pl.BlockSpec((TILE, head), lambda i, s: (lax.rem(i, tiles), 0))
    by_row = lambda cols: pl.BlockSpec((TILE, cols), lambda i, s: (i, 0))
    q_cols = w_query.shape[1]
    return pl.pallas_call(
        functools.partial(qkv_kernel, tiles),
        grid_spec=pltpu.PrefetchScalarGridSpec(
            num_scalar_prefetch=1, grid=(rows // TILE,),
            in_specs=[by_row(width), whole((1, width)), whole(w_query.shape), whole(w_kv.shape), table, table],
            out_specs=[by_row(q_cols), by_row(head), by_row(head)]),
        out_shape=[jax.ShapeDtypeStruct((rows, q_cols), BF16)] + [jax.ShapeDtypeStruct((rows, head), BF16)] * 2,
        compiler_params=pltpu.CompilerParams(**vmem_limit(56)),
        cost_estimate=pl.CostEstimate(flops=2 * rows * width * (q_cols + 2 * head), bytes_accessed=2 * rows * width, transcendentals=0),
    )(seq_lens, x_rows, gain.reshape(1, -1), w_query, w_kv, cos_tab, sin_tab)


def attend(queries, keys, values, seq_lens, order, seq_len):
    q_cols, head = queries.shape[1], keys.shape[1]
    count = order.shape[0]
    by_seq = lambda cols: pl.BlockSpec((seq_len, cols), lambda i, s, o: (o[i], 0))
    return pl.pallas_call(
        attention_kernel,
        grid_spec=pltpu.PrefetchScalarGridSpec(
            num_scalar_prefetch=2, grid=(count,),
            in_specs=[by_seq(q_cols), by_seq(head), by_seq(head)],
            out_specs=[pl.BlockSpec((seq_len, q_cols), lambda i, s, o: (0, 0))] * count),
        out_shape=[jax.ShapeDtypeStruct((seq_len, q_cols), BF16)] * count,
        compiler_params=pltpu.CompilerParams(**vmem_limit(48)),
        cost_estimate=pl.CostEstimate(flops=count * 6 * 10 ** 9, bytes_accessed=count * 2 * 10 ** 6, transcendentals=0),
    )(seq_lens, order, queries, keys, values)


def project_out(pairs, w_full, x_rows, gain, places, first):
    rows, pair_cols = pairs[0].shape
    width = w_full.shape[1]
    tile = 384
    last = len(pairs) - 1
    row_block = pl.BlockSpec((tile, width), lambda i, r, c: (jnp.where(i == last, r, 0), 0))
    return pl.pallas_call(
        out_kernel,
        grid_spec=pltpu.PrefetchScalarGridSpec(
            num_scalar_prefetch=1, grid=(len(pairs), rows // tile),
            in_specs=[pl.BlockSpec((tile, pair_cols), lambda i, r, c, j=j: (jnp.where(i == j, r, 0 if rows == tile else jnp.where(i < j, 0, rows // tile - 1)), 0)) for j in range(len(pairs))]
                     + [pl.BlockSpec((pair_cols, width), lambda i, r, c: (c[1 + i], 0)),
                        pl.BlockSpec((tile, width), lambda i, r, c: ((first + c[0] * rows) // tile + jnp.where(i == last, r, 0), 0)),
                        pl.BlockSpec((1, width), lambda i, r, c: (0, 0))],
            out_specs=[row_block, row_block],
            scratch_shapes=[pltpu.VMEM((rows, width), F32)]),
        out_shape=[jax.ShapeDtypeStruct((rows, width), BF16)] * 2,
        compiler_params=pltpu.CompilerParams(**vmem_limit(62)),
        cost_estimate=pl.CostEstimate(flops=2 * rows * width * len(pairs) * pair_cols, bytes_accessed=4 * width * width, transcendentals=0),
    )(places, *pairs, w_full, x_rows, gain.reshape(1, -1))


def gate_kernel(tiles, mine_ref, other_ref, gate_ref, up_ref, gated_ref):
    step = pl.program_id(0)

    def run(rows_ref):
        gate_pre = jnp.dot(rows_ref[...], gate_ref[...], preferred_element_type=F32)
        up_pre = jnp.dot(rows_ref[...], up_ref[...], preferred_element_type=F32)
        gated_ref[...] = (jax.nn.silu(gate_pre) * up_pre).astype(BF16)

    @pl.when(step < tiles)
    def _():
        run(mine_ref)

    @pl.when(step >= tiles)
    def _():
        run(other_ref)


def gate_up(mine, other, w_gate, w_up):
    rows, width = mine.shape
    hidden = w_gate.shape[1]
    tile = min(rows, 768)
    tiles = rows // tile
    weights = pl.BlockSpec((width, TILE), lambda r, f: (0, f))
    return pl.pallas_call(
        functools.partial(gate_kernel, tiles),
        grid=(2 * tiles, hidden // TILE),
        in_specs=[pl.BlockSpec((tile, width), lambda r, f: (jnp.minimum(r, tiles - 1), 0)),
                  pl.BlockSpec((tile, width), lambda r, f: (jnp.maximum(r - tiles, 0), 0)), weights, weights],
        out_specs=pl.BlockSpec((tile, TILE), lambda r, f: (r, f)),
        out_shape=jax.ShapeDtypeStruct((2 * rows, hidden), BF16),
        compiler_params=pltpu.CompilerParams(**vmem_limit(60)),
        cost_estimate=pl.CostEstimate(flops=8 * rows * width * hidden, bytes_accessed=8 * rows * width, transcendentals=0),
    )(mine, other, w_gate, w_up)


def place_kernel(blocks_ref, *refs):
    refs[-1][...] = blocks_ref[0]


def place_rows(y_rows, blocks, first):
    count, rows, cols = blocks.shape

    def where(k):
        at_y, at_x, core = k // 4, lax.rem(k // 2, 2), lax.rem(k, 2)
        along = jnp.where(core == 0, 2 * at_x + at_y, 2 * at_y + at_x)
        return first + along, core

    fresh = isinstance(y_rows, jax.ShapeDtypeStruct)
    return pl.pallas_call(
        place_kernel,
        grid=(count,),
        in_specs=[pl.BlockSpec((1, rows, cols), lambda k: (k, 0, 0))] + ([] if fresh else [pl.BlockSpec(memory_space=pl.ANY)]),
        out_specs=pl.BlockSpec((rows, cols), where),
        out_shape=jax.ShapeDtypeStruct(y_rows.shape, y_rows.dtype),
        input_output_aliases={} if fresh else {1: 0},
        compiler_params=pltpu.CompilerParams(**vmem_limit(60)),
        cost_estimate=pl.CostEstimate(flops=4 * 10 ** 9, bytes_accessed=2 * blocks.size * 2, transcendentals=0),
    )(blocks, *([] if fresh else [y_rows]))


def after(value, *tokens):
    return lax.optimization_barrier((value,) + tokens)[0]


def solution(mesh):
    tp_size = mesh.shape["tp"]
    sibling = [(i, i ^ 1) for i in range(tp_size)]
    first_axis = [(i, i ^ (4 if i % 2 else 2)) for i in range(tp_size)]
    second_axis = [(i, i ^ (2 if i % 2 else 4)) for i in range(tp_size)]

    def swap(value, pairs):
        return lax.ppermute(value, "tp", pairs)

    def layer_shard(x, seq_lens, w_query, w_key, w_value, w_out, w_gate, w_up, w_down, attn_gain, mlp_gain, k_cache, v_cache):
        batch_size, seq_len, width = x.shape
        head = k_cache.shape[3]
        half = width // 2
        me = lax.axis_index("tp")
        core = me % 2
        at_x = (me // 2) % 2
        at_y = me // 4
        bit_first = jnp.where(core == 0, at_x, at_y)
        bit_second = jnp.where(core == 0, at_y, at_x)
        rows_of = lambda value, index, count: lax.dynamic_slice_in_dim(value, index * count, count, 0)

        w_full = lax.all_gather(w_out, "tp", axis=0, tiled=True)
        x_rows = x.reshape(batch_size * seq_len, width)
        queries, keys, values = project_qkv(x_rows, attn_gain, w_query, jnp.concatenate([w_key, w_value], axis=1), seq_lens, seq_len, head)
        as_cache = lambda rows: rows.reshape(batch_size, seq_len, 1, head)
        k_cache_out = lax.dynamic_update_slice(k_cache, as_cache(keys), (0, 0, 0, 0))
        v_cache_out = lax.dynamic_update_slice(v_cache, as_cache(values), (0, 0, 0, 0))
        down_own = lax.dynamic_slice_in_dim(w_down, core * half, half, 1)
        down_other = lax.dynamic_slice_in_dim(w_down, (1 - core) * half, half, 1)
        chip = me // 2
        along_first = jnp.where(core == 0, 1, 2)
        places = jnp.stack([core, chip, chip ^ along_first, chip ^ (3 - along_first), chip ^ 3]).astype(jnp.int32)

        starts = [sum(PIECES[:p]) for p in range(len(PIECES))]
        count = len(PIECES)
        arrived = []
        lens = seq_lens
        for p in range(count):
            if PIECES[p] == 2:
                mine, give = attend(queries, keys, values, lens, starts[p] + jnp.stack([core, 1 - core]).astype(jnp.int32), seq_len)
            else:
                attn, = attend(queries, keys, values, lens, jnp.full((1,), starts[p], jnp.int32), seq_len)
                mine, give = rows_of(attn, core, seq_len // 2), rows_of(attn, 1 - core, seq_len // 2)
            lens = after(seq_lens, mine)
            heads = jnp.concatenate([mine, swap(give, sibling)], axis=1)
            if p >= 1:
                heads = after(heads, w_full)
            from_first = swap(heads, first_axis)
            from_second = swap(heads, second_axis)
            arrived.append([heads, from_first, from_second, swap(from_first, second_axis)])

        at_keep = bit_first ^ core

        def out_stage(p, places_after):
            rows = PIECES[p] * seq_len
            hidden, normed = project_out(arrived[p], w_full, x_rows, mlp_gain, places_after, starts[p] * seq_len)
            part = lambda row, col: lax.dynamic_slice(hidden, (row * (rows // 4), col * half), (rows // 4, half))
            take = swap(part(bit_first, 1 - core), sibling)
            normed_other = swap(normed, sibling)
            return (normed, normed_other), lambda: jnp.where(bit_first == core, part(bit_second, core), take).astype(F32)

        def place(p, y_rows, blocks):
            return place_rows(y_rows, blocks, starts[p] * seq_len // blocks.shape[1])

        def pair_sum(part_own, from_sibling, at, quarter):
            n = part_own.shape[0] // (2 if quarter is None else 4)
            offset = 0 if quarter is None else quarter * n
            own = lax.dynamic_slice_in_dim(part_own, at * (part_own.shape[0] // 2) + offset, n, 0)
            other = lax.dynamic_slice_in_dim(from_sibling, (1 - at) * (part_own.shape[0] // 2) + offset, n, 0)
            return own.astype(F32) + other.astype(F32)

        def second_stage(parts, got):
            n = got.shape[0] // 2
            send = pair_sum(*parts, at_keep, 1 - bit_second) + rows_of(got, 1 - bit_second, n)
            return send, swap(send, second_axis)

        def finish(residual, parts, got, got_second):
            n = got_second.shape[0]
            total = (pair_sum(*parts, at_keep, bit_second) + rows_of(got, bit_second, n)) + got_second
            mine = (residual() + total).astype(BF16)
            return mine, lax.all_gather(mine, "tp", axis=0)

        y_rows = jax.ShapeDtypeStruct(x_rows.shape, x_rows.dtype)
        normed_rows, residual = out_stage(0, after(places, lens))
        one = two = gathered = None
        for p in range(count):
            gated = gate_up(*normed_rows, w_gate, w_up)
            if one is not None:
                its_residual, parts, got = one
                got = after(got, gated)
                send, got_second = second_stage(parts, got)
                two = (its_residual, parts, got, got_second)
                gated = after(gated, send)
            part_other = jnp.dot(gated, down_other, preferred_element_type=F32).astype(BF16)
            from_sibling = swap(part_other, sibling)
            part_own = jnp.dot(after(gated, part_other), down_own, preferred_element_type=F32).astype(BF16)
            send = pair_sum(part_own, from_sibling, 1 - at_keep, None)
            one = (residual, (part_own, from_sibling), swap(send, first_axis))
            done = send
            if p + 1 < count:
                normed_rows, residual = out_stage(p + 1, after(places, send))
                done = normed_rows[0]
            if gathered is not None:
                y_rows = place(p - 2, y_rows, after(gathered, send))
                gathered = None
            if two is not None:
                its_residual, parts, got, got_second = two
                mine, gathered = finish(its_residual, parts, got, after(got_second, done))
                two = None
                if p + 1 < count:
                    normed_rows = (after(normed_rows[0], mine), normed_rows[1])
        its_residual, parts, got = one
        _, got_second = second_stage(parts, got)
        _, last = finish(its_residual, parts, got, got_second)
        y_rows = place(count - 2, y_rows, gathered)
        y_rows = place(count - 1, y_rows, last)
        return y_rows.reshape(x.shape), k_cache_out, v_cache_out

    cache_spec = P("dp", None, "tp", None)
    return jax.shard_map(layer_shard, mesh=mesh, in_specs=(P("dp", None, None), P("dp"), P(None, "tp"), P(None, "tp"), P(None, "tp"), P("tp", None), P(None, "tp"), P(None, "tp"), P("tp", None), P(), P(), cache_spec, cache_spec), out_specs=(P("dp", None, None), cache_spec, cache_spec), check_vma=False)
```

```python
import functools

import jax
import jax.numpy as jnp
from jax import lax
from jax.experimental import pallas as pl
from jax.experimental.pallas import tpu as pltpu
from jax.sharding import PartitionSpec as P


EPS = 1e-5
ROPE_BASE = 10000.0
F32 = jnp.float32
BF16 = jnp.bfloat16
PIECES = (1,2,2,2,1)
TILE = 256


def rms_rows(rows, gain):
    rows32 = rows.astype(F32)
    inv_rms = lax.rsqrt(jnp.mean(rows32 * rows32, axis=-1, keepdims=True) + EPS)
    return (rows32 * inv_rms * gain.astype(F32)).astype(BF16)


def qkv_kernel(tiles, lens_ref, x_ref, gain_ref, wq_ref, wkv_ref, cos_ref, sin_ref, q_ref, k_ref, v_ref):
    step = pl.program_id(0)
    normed = rms_rows(x_ref[...], gain_ref[...])
    head = cos_ref.shape[1]
    cos_tab = cos_ref[...]
    sin_tab = sin_ref[...]
    even = lax.broadcasted_iota(jnp.int32, cos_tab.shape, 1) % 2 == 0

    def turn(part):
        swapped = jnp.where(even, pltpu.roll(part, head - 1, 1), pltpu.roll(part, 1, 1))
        return (part * cos_tab + swapped * sin_tab).astype(BF16)

    kv = jnp.dot(normed, wkv_ref[...], preferred_element_type=F32)
    rows = lax.rem(step, tiles) * cos_tab.shape[0] + lax.broadcasted_iota(jnp.int32, cos_tab.shape, 0)
    valid = rows < lens_ref[step // tiles]
    zero = jnp.zeros(cos_tab.shape, BF16)
    k_ref[...] = jnp.where(valid, turn(kv[:, :head]), zero)
    v_ref[...] = jnp.where(valid, kv[:, head:].astype(BF16), zero)
    queries = jnp.dot(normed, wq_ref[...], preferred_element_type=F32)
    for h in range(queries.shape[1] // head):
        cols = slice(h * head, (h + 1) * head)
        q_ref[:, cols] = turn(queries[:, cols])


def attention_kernel(lens_ref, seq_ref, q_ref, k_ref, v_ref, *o_refs):
    step = pl.program_id(0)
    length = lens_ref[seq_ref[step]]
    seq_len, head = k_ref.shape
    scale = head ** -0.5

    def run(o_ref):
        for tile in range(seq_len // TILE):
            width = (tile + 1) * TILE
            rows = slice(tile * TILE, (tile + 1) * TILE)
            query_at = tile * TILE + lax.broadcasted_iota(jnp.int32, (TILE, width), 0)
            key_at = lax.broadcasted_iota(jnp.int32, (TILE, width), 1)
            allowed = (key_at <= query_at) & (key_at < length)
            for h in range(q_ref.shape[1] // head):
                cols = slice(h * head, (h + 1) * head)
                scores = lax.dot_general(q_ref[rows, cols], k_ref[:width, :], (((1,), (1,)), ((), ())), preferred_element_type=F32)
                scores = jnp.where(allowed, scores * scale, -jnp.inf)
                top = jnp.max(scores, axis=-1, keepdims=True)
                weights = jnp.exp(scores - top)
                probs = (weights / jnp.sum(weights, axis=-1, keepdims=True)).astype(BF16)
                o_ref[rows, cols] = jnp.dot(probs, v_ref[:width, :], preferred_element_type=F32).astype(BF16)

    for which, o_ref in enumerate(o_refs):
        @pl.when(step == which)
        def _():
            run(o_ref)


def out_kernel(place_ref, *refs):
    pairs, (w_ref, x_ref, gain_ref, h_ref, n_ref, hidden) = refs[:-6], refs[-6:]
    step = pl.program_id(0)
    core = place_ref[0]
    depth = w_ref.shape[0] // (2 * len(pairs))
    rows, cols = x_ref.shape
    total = None
    for which, o_ref in enumerate(pairs):
        for k, owner in enumerate((core, 1 - core)):
            group = 2 * place_ref[1 + which] + owner
            part = jnp.dot(o_ref[:, k * depth:(k + 1) * depth], w_ref[pl.ds(pl.multiple_of(group * depth, depth), depth), :], preferred_element_type=F32).astype(BF16)
            total = part.astype(F32) if total is None else total + part.astype(F32)
    h = (x_ref[...].astype(F32) + total).astype(BF16)
    h_ref[...] = h
    hidden[:, pl.ds(pl.multiple_of(step * cols, cols), cols)] = h

    @pl.when(step == pl.num_programs(0) - 1)
    def _():
        for row in range(0, rows, 128):
            n_ref[row:row + 128, :] = rms_rows(hidden[row:row + 128, :], gain_ref[...])


def rope_tables(seq_len, head):
    inv_freq = ROPE_BASE ** (-jnp.arange(0, head, 2).astype(F32) / head)
    angles = jnp.arange(seq_len).astype(F32)[:, None] * inv_freq[None, :]
    sign = jnp.where(jnp.arange(head) % 2 == 0, -1.0, 1.0).astype(F32)
    return jnp.repeat(jnp.cos(angles), 2, axis=1), jnp.repeat(jnp.sin(angles), 2, axis=1) * sign


def vmem_limit(mib):
    return dict(vmem_limit_bytes=mib * 2 ** 20)


def project_qkv(x_rows, gain, w_query, w_kv, seq_lens, seq_len, head):
    rows, width = x_rows.shape
    tiles = seq_len // TILE
    cos_tab, sin_tab = rope_tables(seq_len, head)
    whole = lambda shape: pl.BlockSpec(shape, lambda i, s: (0, 0))
    table = pl.BlockSpec((TILE, head), lambda i, s: (lax.rem(i, tiles), 0))
    by_row = lambda cols: pl.BlockSpec((TILE, cols), lambda i, s: (i, 0))
    q_cols = w_query.shape[1]
    return pl.pallas_call(
        functools.partial(qkv_kernel, tiles),
        grid_spec=pltpu.PrefetchScalarGridSpec(
            num_scalar_prefetch=1, grid=(rows // TILE,),
            in_specs=[by_row(width), whole((1, width)), whole(w_query.shape), whole(w_kv.shape), table, table],
            out_specs=[by_row(q_cols), by_row(head), by_row(head)]),
        out_shape=[jax.ShapeDtypeStruct((rows, q_cols), BF16)] + [jax.ShapeDtypeStruct((rows, head), BF16)] * 2,
        compiler_params=pltpu.CompilerParams(**vmem_limit(56)),
        cost_estimate=pl.CostEstimate(flops=2 * rows * width * (q_cols + 2 * head), bytes_accessed=2 * rows * width, transcendentals=0),
    )(seq_lens, x_rows, gain.reshape(1, -1), w_query, w_kv, cos_tab, sin_tab)


def attend(queries, keys, values, seq_lens, order, seq_len):
    q_cols, head = queries.shape[1], keys.shape[1]
    count = order.shape[0]
    by_seq = lambda cols: pl.BlockSpec((seq_len, cols), lambda i, s, o: (o[i], 0))
    return pl.pallas_call(
        attention_kernel,
        grid_spec=pltpu.PrefetchScalarGridSpec(
            num_scalar_prefetch=2, grid=(count,),
            in_specs=[by_seq(q_cols), by_seq(head), by_seq(head)],
            out_specs=[pl.BlockSpec((seq_len, q_cols), lambda i, s, o: (0, 0))] * count),
        out_shape=[jax.ShapeDtypeStruct((seq_len, q_cols), BF16)] * count,
        compiler_params=pltpu.CompilerParams(**vmem_limit(48)),
        cost_estimate=pl.CostEstimate(flops=count * 6 * 10 ** 9, bytes_accessed=count * 2 * 10 ** 6, transcendentals=0),
    )(seq_lens, order, queries, keys, values)


def project_out(pairs, w_full, x_rows, gain, places, first):
    rows, pair_cols = pairs[0].shape
    width = w_full.shape[1]
    cols = 512
    return pl.pallas_call(
        out_kernel,
        grid_spec=pltpu.PrefetchScalarGridSpec(
            num_scalar_prefetch=1, grid=(width // cols,),
            in_specs=[pl.BlockSpec((rows, pair_cols), lambda n, c: (0, 0))] * len(pairs)
                     + [pl.BlockSpec((width, cols), lambda n, c: (0, n)),
                        pl.BlockSpec((rows, cols), lambda n, c: (first // rows + c[0], n)),
                        pl.BlockSpec((1, width), lambda n, c: (0, 0))],
            out_specs=[pl.BlockSpec((rows, cols), lambda n, c: (0, n)), pl.BlockSpec((rows, width), lambda n, c: (0, 0))],
            scratch_shapes=[pltpu.VMEM((rows, width), BF16)]),
        out_shape=[jax.ShapeDtypeStruct((rows, width), BF16)] * 2,
        compiler_params=pltpu.CompilerParams(**vmem_limit(62)),
        cost_estimate=pl.CostEstimate(flops=2 * rows * width * len(pairs) * pair_cols, bytes_accessed=4 * width * width, transcendentals=0),
    )(places, *pairs, w_full, x_rows, gain.reshape(1, -1))


def gate_kernel(tiles, mine_ref, other_ref, gate_ref, up_ref, gated_ref):
    step = pl.program_id(0)

    def run(rows_ref):
        gate_pre = jnp.dot(rows_ref[...], gate_ref[...], preferred_element_type=F32)
        up_pre = jnp.dot(rows_ref[...], up_ref[...], preferred_element_type=F32)
        gated_ref[...] = (jax.nn.silu(gate_pre) * up_pre).astype(BF16)

    @pl.when(step < tiles)
    def _():
        run(mine_ref)

    @pl.when(step >= tiles)
    def _():
        run(other_ref)


def gate_up(mine, other, w_gate, w_up):
    rows, width = mine.shape
    hidden = w_gate.shape[1]
    tile = min(rows, 768)
    tiles = rows // tile
    weights = pl.BlockSpec((width, TILE), lambda r, f: (0, f))
    return pl.pallas_call(
        functools.partial(gate_kernel, tiles),
        grid=(2 * tiles, hidden // TILE),
        in_specs=[pl.BlockSpec((tile, width), lambda r, f: (jnp.minimum(r, tiles - 1), 0)),
                  pl.BlockSpec((tile, width), lambda r, f: (jnp.maximum(r - tiles, 0), 0)), weights, weights],
        out_specs=pl.BlockSpec((tile, TILE), lambda r, f: (r, f)),
        out_shape=jax.ShapeDtypeStruct((2 * rows, hidden), BF16),
        compiler_params=pltpu.CompilerParams(**vmem_limit(60)),
        cost_estimate=pl.CostEstimate(flops=8 * rows * width * hidden, bytes_accessed=8 * rows * width, transcendentals=0),
    )(mine, other, w_gate, w_up)


def place_kernel(blocks_ref, *refs):
    refs[-1][...] = blocks_ref[0]


def place_rows(y_rows, blocks, first):
    count, rows, cols = blocks.shape

    def where(k):
        at_y, at_x, core = k // 4, lax.rem(k // 2, 2), lax.rem(k, 2)
        along = jnp.where(core == 0, 2 * at_x + at_y, 2 * at_y + at_x)
        return first + along, core

    fresh = isinstance(y_rows, jax.ShapeDtypeStruct)
    return pl.pallas_call(
        place_kernel,
        grid=(count,),
        in_specs=[pl.BlockSpec((1, rows, cols), lambda k: (k, 0, 0))] + ([] if fresh else [pl.BlockSpec(memory_space=pl.ANY)]),
        out_specs=pl.BlockSpec((rows, cols), where),
        out_shape=jax.ShapeDtypeStruct(y_rows.shape, y_rows.dtype),
        input_output_aliases={} if fresh else {1: 0},
        compiler_params=pltpu.CompilerParams(**vmem_limit(60)),
        cost_estimate=pl.CostEstimate(flops=4 * 10 ** 9, bytes_accessed=2 * blocks.size * 2, transcendentals=0),
    )(blocks, *([] if fresh else [y_rows]))


def after(value, *tokens):
    return lax.optimization_barrier((value,) + tokens)[0]


def solution(mesh):
    tp_size = mesh.shape["tp"]
    sibling = [(i, i ^ 1) for i in range(tp_size)]
    first_axis = [(i, i ^ (4 if i % 2 else 2)) for i in range(tp_size)]
    second_axis = [(i, i ^ (2 if i % 2 else 4)) for i in range(tp_size)]

    def swap(value, pairs):
        return lax.ppermute(value, "tp", pairs)

    def layer_shard(x, seq_lens, w_query, w_key, w_value, w_out, w_gate, w_up, w_down, attn_gain, mlp_gain, k_cache, v_cache):
        batch_size, seq_len, width = x.shape
        head = k_cache.shape[3]
        half = width // 2
        me = lax.axis_index("tp")
        core = me % 2
        at_x = (me // 2) % 2
        at_y = me // 4
        bit_first = jnp.where(core == 0, at_x, at_y)
        bit_second = jnp.where(core == 0, at_y, at_x)
        rows_of = lambda value, index, count: lax.dynamic_slice_in_dim(value, index * count, count, 0)

        w_full = lax.all_gather(w_out, "tp", axis=0, tiled=True)
        x_rows = x.reshape(batch_size * seq_len, width)
        queries, keys, values = project_qkv(x_rows, attn_gain, w_query, jnp.concatenate([w_key, w_value], axis=1), seq_lens, seq_len, head)
        as_cache = lambda rows: rows.reshape(batch_size, seq_len, 1, head)
        k_cache_out = lax.dynamic_update_slice(k_cache, as_cache(keys), (0, 0, 0, 0))
        v_cache_out = lax.dynamic_update_slice(v_cache, as_cache(values), (0, 0, 0, 0))
        down_own = lax.dynamic_slice_in_dim(w_down, core * half, half, 1)
        down_other = lax.dynamic_slice_in_dim(w_down, (1 - core) * half, half, 1)
        chip = me // 2
        along_first = jnp.where(core == 0, 1, 2)
        places = jnp.stack([core, chip, chip ^ along_first, chip ^ (3 - along_first), chip ^ 3]).astype(jnp.int32)

        starts = [sum(PIECES[:p]) for p in range(len(PIECES))]
        count = len(PIECES)
        arrived = []
        lens = seq_lens
        for p in range(count):
            if PIECES[p] == 2:
                mine, give = attend(queries, keys, values, lens, starts[p] + jnp.stack([core, 1 - core]).astype(jnp.int32), seq_len)
            else:
                attn, = attend(queries, keys, values, lens, jnp.full((1,), starts[p], jnp.int32), seq_len)
                mine, give = rows_of(attn, core, seq_len // 2), rows_of(attn, 1 - core, seq_len // 2)
            lens = after(seq_lens, mine)
            heads = jnp.concatenate([mine, swap(give, sibling)], axis=1)
            if p >= 1:
                heads = after(heads, w_full)
            from_first = swap(heads, first_axis)
            from_second = swap(heads, second_axis)
            arrived.append([heads, from_first, from_second, swap(from_first, second_axis)])

        at_keep = bit_first ^ core

        def out_stage(p, places_after):
            rows = PIECES[p] * seq_len
            hidden, normed = project_out(arrived[p], w_full, x_rows, mlp_gain, places_after, starts[p] * seq_len)
            part = lambda row, col: lax.dynamic_slice(hidden, (row * (rows // 4), col * half), (rows // 4, half))
            take = swap(part(bit_first, 1 - core), sibling)
            normed_other = swap(normed, sibling)
            return (normed, normed_other), lambda: jnp.where(bit_first == core, part(bit_second, core), take).astype(F32)

        def place(p, y_rows, blocks):
            return place_rows(y_rows, blocks, starts[p] * seq_len // blocks.shape[1])

        def pair_sum(part_own, from_sibling, at, quarter):
            n = part_own.shape[0] // (2 if quarter is None else 4)
            offset = 0 if quarter is None else quarter * n
            own = lax.dynamic_slice_in_dim(part_own, at * (part_own.shape[0] // 2) + offset, n, 0)
            other = lax.dynamic_slice_in_dim(from_sibling, (1 - at) * (part_own.shape[0] // 2) + offset, n, 0)
            return own.astype(F32) + other.astype(F32)

        def second_stage(parts, got):
            n = got.shape[0] // 2
            send = pair_sum(*parts, at_keep, 1 - bit_second) + rows_of(got, 1 - bit_second, n)
            return send, swap(send, second_axis)

        def finish(residual, parts, got, got_second):
            n = got_second.shape[0]
            total = (pair_sum(*parts, at_keep, bit_second) + rows_of(got, bit_second, n)) + got_second
            mine = (residual() + total).astype(BF16)
            return mine, lax.all_gather(mine, "tp", axis=0)

        y_rows = jax.ShapeDtypeStruct(x_rows.shape, x_rows.dtype)
        normed_rows, residual = out_stage(0, after(places, lens))
        one = two = gathered = None
        for p in range(count):
            gated = gate_up(*normed_rows, w_gate, w_up)
            if one is not None:
                its_residual, parts, got = one
                got = after(got, gated)
                send, got_second = second_stage(parts, got)
                two = (its_residual, parts, got, got_second)
                gated = after(gated, send)
            part_other = jnp.dot(gated, down_other, preferred_element_type=F32).astype(BF16)
            from_sibling = swap(part_other, sibling)
            part_own = jnp.dot(after(gated, part_other), down_own, preferred_element_type=F32).astype(BF16)
            send = pair_sum(part_own, from_sibling, 1 - at_keep, None)
            one = (residual, (part_own, from_sibling), swap(send, first_axis))
            done = send
            if p + 1 < count:
                normed_rows, residual = out_stage(p + 1, after(places, send))
                done = normed_rows[0]
            if gathered is not None:
                y_rows = place(p - 2, y_rows, after(gathered, send))
                gathered = None
            if two is not None:
                its_residual, parts, got, got_second = two
                mine, gathered = finish(its_residual, parts, got, after(got_second, done))
                two = None
                if p + 1 < count:
                    normed_rows = (after(normed_rows[0], mine), normed_rows[1])
        its_residual, parts, got = one
        _, got_second = second_stage(parts, got)
        _, last = finish(its_residual, parts, got, got_second)
        y_rows = place(count - 2, y_rows, gathered)
        y_rows = place(count - 1, y_rows, last)
        return y_rows.reshape(x.shape), k_cache_out, v_cache_out

    cache_spec = P("dp", None, "tp", None)
    return jax.shard_map(layer_shard, mesh=mesh, in_specs=(P("dp", None, None), P("dp"), P(None, "tp"), P(None, "tp"), P(None, "tp"), P("tp", None), P(None, "tp"), P(None, "tp"), P("tp", None), P(), P(), cache_spec, cache_spec), out_specs=(P("dp", None, None), cache_spec, cache_spec), check_vma=False)
```
